256 devices in a mesh: dp: 8 (over y, x_lo), tensor: 16 (over z, core), fisher: 2 (over x_hi).
Axes of the slice: x: 4 (x_hi: 2, x_lo: 2; x = x_hi * 2 + x_lo), y: 4, z: 8, core: 2. Of those that a mesh axis runs over, the one named last changes fastest.
Arguments:
- train_inputs: bfloat16 [176, 257, 1280], P('dp', None, 'fisher'), may hold values from -6 to 6
- train_cotangents: bfloat16 [176, 257, 3840], P('dp', None, 'tensor'), may hold values from -6 to 6
- train_ids: int32 [176], P('dp'), may hold values from 0 to 63
- query_projection_inputs: bfloat16 [16, 257, 1280], P('tensor', None, 'fisher'), may hold values from -6 to 6
- query_output_cotangents: bfloat16 [16, 257, 3840], P('tensor'), may hold values from -6 to 6
- query_ids: int32 [16], replicated, may hold values from 0 to 15
- fisher_diagonal_weight: bfloat16 [2, 3840, 1280], P(None, 'tensor', 'fisher'), may hold values from 0.049804688 to 2
- layer_index: int32 [16], replicated, may hold values from 0 to 1
Outputs:
- influence: float32 [64, 16, 16], P(('dp', 'fisher'), None, 'tensor')
The draws below stay inside these ranges and needn't reach their ends.
All inputs are finite; a program needn't handle non-finite values.
Results may differ from the reference program's by a relative error of at most 0.004.
Values may be sent and summed in bfloat16 or wider, within the bound.
No kernel may reach another device: no remote copies, remote signals or barrier semaphores. Data moves between devices by JAX's collectives and lax.ppermute only.
A program may use at most 128 MiB of HBM per device.

```python
import math
import jax
import jax.numpy as jnp
from jax import lax

D = 1280
HEADS = 16
HEAD_DIM = 80
SEQ = 257
QIDS = 16
LAYERS = 2
TRAIN = 176
QUERIES = 16
TIDS = 64


def plant(drawn, rng, least, top_value):
    longest = drawn.shape.index(max(drawn.shape))
    spots = []
    for shift in (0, 1):
        where = [jax.random.randint(jax.random.fold_in(rng, axis), (), 0, length) for axis, length in enumerate(drawn.shape)]
        where[longest] = (where[longest] + shift) % drawn.shape[longest]
        spots.append(tuple(where))
    return drawn.at[spots[0]].set(least).at[spots[1]].set(top_value)


def block_scale(own_key, extent, pieces, low, high):
    factor_of, own = 1.0, jax.random.fold_in(own_key, 6)
    for axis_at, blocks in pieces:
        heights = jnp.exp(jax.random.uniform(jax.random.fold_in(own, axis_at), (blocks,), jnp.float32, low / len(pieces), high / len(pieces)))
        factor_of = factor_of * jnp.repeat(heights, extent[axis_at] // blocks).reshape([-1 if axis == axis_at else 1 for axis in range(len(extent))])
    return factor_of


def centred(key, extent, width, limit, split=(), held_as=jnp.bfloat16):
    drawn = jax.random.normal(key, extent, jnp.float32) * width
    if len(split) > 0:
        drawn = block_scale(key, extent, split, -0.22, 0.18) * drawn
    return jnp.clip(drawn, min=-limit, max=limit).astype(held_as)


def setup_inputs(seed: int = 0) -> dict:
    key_of = jax.random.split(jax.random.key(seed), 9)
    train_inputs = centred(key_of[0], (TRAIN, SEQ, D), 1.0, 6.0, ((0, 8), (2, 2)))
    train_cotangents = centred(key_of[1], (TRAIN, SEQ, 3 * HEADS * HEAD_DIM), 1.0, 6.0, ((0, 8), (2, 16)))
    train_ids = plant(jax.random.randint(key_of[2], (TRAIN,), 0, TIDS), jax.random.fold_in(key_of[2], 1), 0, TIDS - 1).astype(jnp.int32)
    query_projection_inputs = centred(key_of[3], (QUERIES, SEQ, D), 1.0, 6.0, ((0, 16), (2, 2)))
    query_output_cotangents = centred(key_of[4], (QUERIES, SEQ, 3 * HEADS * HEAD_DIM), 1.0, 6.0, ((0, 16),))
    query_ids = plant(jax.random.randint(key_of[5], (QUERIES,), 0, QIDS), jax.random.fold_in(key_of[5], 1), 0, QIDS - 1).astype(jnp.int32)
    fisher_diagonal_weight = jnp.clip(jnp.exp(math.log(2.0) - 3.6927934 * jax.random.uniform(key_of[6], (LAYERS, 3 * HEADS * HEAD_DIM, D), jnp.float32) ** block_scale(key_of[6], (LAYERS, 3 * HEADS * HEAD_DIM, D), ((1, 16), (2, 2)), -0.2, 0.2)), 0.049804688, 2.0).astype(jnp.bfloat16)
    layer_index = plant(jax.random.randint(key_of[7], (HEADS,), 0, LAYERS), jax.random.fold_in(key_of[7], 1), 0, LAYERS - 1).astype(jnp.int32)
    return dict(train_inputs=train_inputs, train_cotangents=train_cotangents, train_ids=train_ids, query_projection_inputs=query_projection_inputs, query_output_cotangents=query_output_cotangents, query_ids=query_ids, fisher_diagonal_weight=fisher_diagonal_weight, layer_index=layer_index)


def reference(train_inputs, train_cotangents, train_ids, query_projection_inputs, query_output_cotangents, query_ids, fisher_diagonal_weight, layer_index):
    head_width = 3 * HEAD_DIM
    scale_factor = 1.0 / (SEQ * math.sqrt(3 * HEAD_DIM * D))
    stacked = fisher_diagonal_weight.astype(jnp.float32).reshape(LAYERS, HEADS, head_width, D)
    picked = (layer_index[None, :] == jnp.arange(LAYERS, dtype=jnp.int32)[:, None]).astype(jnp.float32)
    fisher_heads = lax.optimization_barrier(jnp.sum(stacked * picked[:, :, None, None], axis=0))
    train_act = train_inputs.astype(jnp.float32)
    query_activation = query_projection_inputs.astype(jnp.float32)
    train_cot = jnp.moveaxis(train_cotangents.astype(jnp.float32).reshape(TRAIN, SEQ, HEADS, head_width), 2, 0)
    query_cot = jnp.moveaxis(query_output_cotangents.astype(jnp.float32).reshape(QUERIES, SEQ, HEADS, head_width), 2, 0)

    def per_head(operands):
        train_part, query_portion, fisher_part = operands
        train_grad = jnp.einsum('nsr,nsd->nrd', train_part, train_act).astype(jnp.bfloat16)
        query_gradient = jnp.einsum('kzo,kzj->koj', query_portion, query_activation)
        weighted = (fisher_part[None] * query_gradient).astype(jnp.bfloat16)
        return jnp.einsum('nx,mx->nm', train_grad.reshape(TRAIN, -1).astype(jnp.float32), weighted.reshape(QUERIES, -1).astype(jnp.float32))
    scores = lax.map(per_head, (train_cot, query_cot, fisher_heads)) * scale_factor
    train_hot = (train_ids[:, None] == jnp.arange(TIDS, dtype=jnp.int32)[None, :]).astype(jnp.float32)
    query_hot = (query_ids[:, None] == jnp.arange(QIDS, dtype=jnp.int32)[None, :]).astype(jnp.float32)
    return jnp.einsum('hnm,na,mb->abh', scores, train_hot, query_hot, precision=lax.Precision.HIGHEST)
```

```python
import math

import jax
import jax.numpy as jnp
from jax import lax
from jax.sharding import Mesh, PartitionSpec as P

D = 1280
HEAD_DIM = 80
SEQ = 257
TIDS = 64
QIDS = 16
HW = 3 * HEAD_DIM
NY, NXL, NZ, NC, NXH = 4, 2, 8, 2, 2
AXES = ("y", "xlo", "z", "core", "xhi")


def flat(y, x, z, c):
    return (((y % 4) * NXL + (x % 4) % 2) * NZ + z % NZ) * NC * NXH + (c % 2) * NXH + (x % 4) // 2


def places():
    return [(y, x, z, c) for y in range(4) for x in range(4) for z in range(NZ) for c in range(2)]


def send(value, to):
    perm = [(flat(*p), flat(*to(*p))) for p in places()]
    return lax.ppermute(value, AXES, perm)


def offset_of(y, x):
    return (2 * y + x // 2) % 8


def local(
    train_inputs,
    train_cotangents,
    train_ids,
    query_projection_inputs,
    query_output_cotangents,
    query_ids,
    fisher_diagonal_weight,
    layer_index,
):
    scale_factor = 1.0 / (SEQ * math.sqrt(HW * D))
    half_width = train_inputs.shape[2]
    core = lax.axis_index("core")
    z = lax.axis_index("z")
    y = lax.axis_index("y")
    x = lax.axis_index("xhi") * 2 + lax.axis_index("xlo")

    own_x = query_projection_inputs[0]
    up = lambda y, x, z, c: (y, x, z + 1, c)
    down = lambda y, x, z, c: (y, x, z - 1, c)
    m1 = send(own_x, up)
    p1 = send(own_x, down)

    a = (2 * y + x // 2 + 4 * core) % 8
    head = 2 * ((z - a) % 8) + x % 2
    cot = query_output_cotangents[0]
    unit = lax.dynamic_slice_in_dim(cot, head * HW, HW, 1)
    unit = send(unit, lambda y, x, z, c: (y, x, z - offset_of(y, x) - 4 * c, c))

    def turn(k, first):
        def to(y, x, z, c):
            return (y, x - k, z, c) if (c == 0) == first else (y - k, x, z, c)
        return to

    line = jnp.stack([unit, send(unit, turn(1, True)), send(unit, turn(-1, True)), send(unit, turn(2, True))])
    m2 = send(m1, up)
    p2 = send(p1, down)
    lp = send(line, turn(1, False))
    lm = send(line, turn(-1, False))
    l2a = send(lp[:2], turn(1, False))
    l2b = send(lm[2:], turn(-1, False))
    units = jnp.concatenate([line, lp, lm, l2a, l2b])
    m3 = send(m2, up)
    p3 = send(p2, down)
    far = lax.select(core == 0, m3, p3)
    f4 = send(far, lambda y, x, z, c: (y, x, z + 1 - 2 * c, c))
    queries = jnp.stack([own_x, p1, p2, p3, f4, m3, m2, m1])

    steps = jnp.array([0, 1, -1, 2], jnp.int32)
    k_in, k_out = jnp.meshgrid(steps, steps, indexing="ij")
    slot_in, slot_out = k_in.T.reshape(16), k_out.T.reshape(16)
    ux = (x + jnp.where(core == 0, slot_in, slot_out)) % 4
    uy = (y + jnp.where(core == 0, slot_out, slot_in)) % 4
    u_off = (2 * uy + ux // 2 + 4 * core) % 8
    u_key = u_off + 8 * ((ux % 2) ^ core)
    want = jnp.arange(16, dtype=jnp.int32)
    index = jnp.sum(jnp.where(u_key[None, :] == want[:, None], jnp.arange(16, dtype=jnp.int32)[None, :], 0), axis=1)
    cots = jnp.take(units, index, axis=0, mode="clip")

    own_layer = lax.dynamic_slice_in_dim(layer_index, 2 * z + core, 1, 0)
    picked = own_layer == jnp.arange(fisher_diagonal_weight.shape[0], dtype=jnp.int32)
    fisher_own = jnp.sum(
        jnp.where(picked[:, None, None], fisher_diagonal_weight.astype(jnp.float32), 0.0), axis=0
    ).astype(jnp.bfloat16)
    swap = lambda y, x, z, c: (y, x, z, 1 - c)
    fisher = jnp.stack([fisher_own, send(fisher_own, swap)]).astype(jnp.float32)

    grad_own = jnp.einsum(
        "nsr,nsd->nrd", train_cotangents, train_inputs, preferred_element_type=jnp.float32
    ).astype(jnp.bfloat16)
    grad_other = send(grad_own, swap)

    def scores_of(grad, e):
        block = jnp.einsum(
            "kzo,kzj->koj", cots[8 * e : 8 * e + 8], queries, preferred_element_type=jnp.float32
        )
        weighted = (fisher[e][None] * block).astype(jnp.bfloat16)
        return lax.dot_general(
            grad.reshape(grad.shape[0], HW * half_width),
            weighted.reshape(8, HW * half_width),
            (((1,), (1,)), ((), ())),
            preferred_element_type=jnp.float32,
        ) * scale_factor

    scores = jnp.stack([scores_of(grad_own, 0), scores_of(grad_other, 1)])
    train_hot = (train_ids[:, None] == jnp.arange(TIDS, dtype=jnp.int32)[None, :]).astype(jnp.float32)
    order = 2 * ((z + jnp.arange(8, dtype=jnp.int32)) % 8) + core
    ids = jnp.take(query_ids, order, mode="clip")
    query_hot = (ids[:, None] == jnp.arange(QIDS, dtype=jnp.int32)[None, :]).astype(jnp.float32)
    buckets = jnp.einsum(
        "hnm,na,mb->hab", scores, train_hot, query_hot, precision=lax.Precision.HIGHEST
    )
    buckets = buckets[0] + send(buckets[1], swap)
    shares = lax.all_to_all(
        buckets.reshape(NY * NXL * NXH, 4, QIDS), ("y", "xlo", "xhi"), 0, 0, tiled=True
    )
    return jnp.sum(shares, axis=0)[:, :, None]


def solution(mesh):
    fine = Mesh(mesh.devices.reshape(NY, NXL, NZ, NC, NXH), AXES)
    dp, tensor, fisher = ("y", "xlo"), ("z", "core"), "xhi"
    in_specs = (
        P(dp, None, fisher),
        P(dp, None, tensor),
        P(dp),
        P(tensor, None, fisher),
        P(tensor, None, None),
        P(),
        P(None, tensor, fisher),
        P(),
    )
    out_specs = P(("y", "xlo", "xhi"), None, tensor)
    return jax.shard_map(local, mesh=fine, in_specs=in_specs, out_specs=out_specs, check_vma=False)
```

```python
import functools
import math

import jax
import jax.numpy as jnp
from jax import lax
from jax.experimental import pallas as pl
from jax.experimental.pallas import tpu as pltpu
from jax.sharding import Mesh, PartitionSpec as P

D = 1280
HEAD_DIM = 80
SEQ = 257
BODY = 256
TIDS = 64
QIDS = 16
HW = 3 * HEAD_DIM
HALF = D // 2
ROWS = 16
NY, NXL, NZ, NC, NXH = 4, 2, 8, 2, 2
AXES = ("y", "xlo", "z", "core", "xhi")
CUTS = (11, 11)
SCALE = 1.0 / (SEQ * math.sqrt(HW * D))
ANY = pl.BlockSpec(memory_space=pl.ANY)
VMEM = pl.BlockSpec(memory_space=pltpu.VMEM)
SMEM = pl.BlockSpec(memory_space=pltpu.SMEM)


def flat(y, x, z, c):
    return (((y % 4) * NXL + (x % 4) % 2) * NZ + z % NZ) * NC * NXH + (c % 2) * NXH + (x % 4) // 2


def send(value, to):
    places = [(y, x, z, c) for y in range(4) for x in range(4) for z in range(NZ) for c in range(2)]
    return lax.ppermute(value, AXES, [(flat(*p), flat(*to(*p))) for p in places])


def outer_sum(cot, act):
    body = lax.dot_general(
        cot[:BODY], act[:BODY], (((0,), (0,)), ((), ())), preferred_element_type=jnp.float32
    )
    column = jnp.transpose(cot[BODY:SEQ].astype(jnp.float32))
    return body + column * act[BODY:SEQ].astype(jnp.float32)


def train_kernel(first, group, cot_hbm, act_hbm, out_ref, cot, act, sems):
    count = out_ref.shape[0]
    copies = []
    for i in range(0, count, group):
        size = min(group, count - i)
        src, dst = pl.ds(first + i, size), pl.ds(i, size)
        pair = (
            pltpu.make_async_copy(cot_hbm.at[src], cot.at[dst], sems.at[0, i // group]),
            pltpu.make_async_copy(act_hbm.at[src], act.at[dst], sems.at[1, i // group]),
        )
        copies.append((i, size, pair))
        for c in pair:
            c.start()
    for i, size, pair in copies:
        for c in pair:
            c.wait()
        for j in range(i, i + size):
            out_ref[j] = outer_sum(cot[j], act[j]).astype(jnp.bfloat16)


def train_grad(cot, act, first, count):
    group = 2
    return pl.pallas_call(
        functools.partial(train_kernel, first, group),
        in_specs=[ANY, ANY],
        out_specs=VMEM,
        out_shape=jax.ShapeDtypeStruct((count, HW, HALF), jnp.bfloat16),
        scratch_shapes=[
            pltpu.VMEM((count, SEQ, HW), jnp.bfloat16),
            pltpu.VMEM((count, SEQ, HALF), jnp.bfloat16),
            pltpu.SemaphoreType.DMA((2, -(-count // group))),
        ],
        name="train_grad",
        compiler_params=pltpu.CompilerParams(vmem_limit_bytes=58 * 2**20),
        cost_estimate=pl.CostEstimate(
            flops=2 * count * HW * HALF * SEQ * 4,
            bytes_accessed=2 * count * (SEQ * (HW + HALF) + HW * HALF),
            transcendentals=0,
        ),
    )(cot, act)


def stack_kernel(*refs):
    *sources, out = refs
    for i, ref in enumerate(sources):
        out[i] = ref[...]


def stack(*parts):
    return pl.pallas_call(
        stack_kernel,
        in_specs=[VMEM] * len(parts),
        out_specs=VMEM,
        out_shape=jax.ShapeDtypeStruct((len(parts),) + parts[0].shape, parts[0].dtype),
        name="stack",
        compiler_params=pltpu.CompilerParams(vmem_limit_bytes=4 * 2**20),
    )(*parts)


def pair_kernel(count_train, *refs):
    acts, refs = refs[:8], refs[8:]
    cots, refs = refs[:8], refs[8:]
    grads, refs = refs[:4], refs[4:]
    own_fisher, other_fisher, ids_ref, query_ids, layer_index, out_ref = refs[:6]
    cot, grad, weighted, act, sems = refs[6:]
    core, z, y = lax.axis_index("core"), lax.axis_index("z"), lax.axis_index("y")
    x = lax.axis_index("xhi") * 2 + lax.axis_index("xlo")
    first, later = [], []
    for k, ref in enumerate(acts):
        first.append(pltpu.make_async_copy(ref, act.at[k], sems.at[k]))
    for i, ref in enumerate(cots):
        first.append(pltpu.make_async_copy(ref, cot.at[pl.ds(2 * i, 2)], sems.at[8 + i]))
    for i, ref in enumerate(grads):
        rows = pl.ds((i % 2) * CUTS[0], ref.shape[0])
        later.append(pltpu.make_async_copy(ref, grad.at[i // 2, rows], sems.at[16 + i]))
    for c in first + later:
        c.start()
    train_hot = (
        lax.broadcasted_iota(jnp.int32, (TIDS, count_train), 0) == ids_ref[...]
    ).astype(jnp.float32)
    column = lax.broadcasted_iota(jnp.int32, (8 * ROWS, QIDS), 0)
    wanted = jnp.zeros((8 * ROWS, QIDS), jnp.int32)
    for k in range(8):
        one = query_ids[2 * lax.rem(z + k, 8) + core]
        wanted = jnp.where(column // ROWS == k, one, wanted)
    query_hot = (lax.broadcasted_iota(jnp.int32, (8 * ROWS, QIDS), 1) == wanted).astype(jnp.float32)
    row = lax.broadcasted_iota(jnp.int32, (count_train * ROWS, 8 * ROWS), 0)
    col = lax.broadcasted_iota(jnp.int32, (count_train * ROWS, 8 * ROWS), 1)
    same = lax.rem(row, ROWS) == lax.rem(col, ROWS)

    def slot(d):
        d = lax.rem(d + 4, 4)
        return jnp.where(d == 2, 3, jnp.where(d == 3, 2, d))

    for c in first:
        c.wait()
    for e in range(2):
        parity = core if e == 0 else 1 - core
        fisher_ref = own_fisher if e == 0 else other_fisher
        fisher = fisher_ref[layer_index[2 * z + parity]].astype(jnp.float32)
        for k in range(8):
            t = lax.rem(k + 4 * core, 8)
            dy, dx = slot(t // 2 - y), slot(lax.rem(t, 2) * 2 + parity - x)
            unit = jnp.where(core == 0, dy * 4 + dx, dx * 4 + dy)
            weighted[k] = (fisher * outer_sum(cot[unit], act[k])).astype(jnp.bfloat16)
        for c in later[2 * e : 2 * e + 2]:
            c.wait()
        total = jnp.zeros((count_train * ROWS, 8 * ROWS), jnp.float32)
        for r in range(0, HW, ROWS):
            lhs = grad[e, :, r : r + ROWS, :].reshape(count_train * ROWS, HALF)
            rhs = weighted[:, r : r + ROWS, :].reshape(8 * ROWS, HALF)
            total += lax.dot_general(
                lhs, rhs, (((1,), (1,)), ((), ())), preferred_element_type=jnp.float32
            )
        total = jnp.where(same, total, 0.0).reshape(count_train, ROWS, 8 * ROWS).sum(axis=1) * SCALE
        total = jnp.dot(
            total, query_hot, precision=lax.Precision.HIGHEST, preferred_element_type=jnp.float32
        )
        out_ref[e] = jnp.dot(
            train_hot, total, precision=lax.Precision.HIGHEST, preferred_element_type=jnp.float32
        )


def pair_scores(acts, cots, own_grads, other_grads, own_fisher, other_fisher, ids, query_ids, layers):
    count = ids.shape[0]
    bf = jnp.bfloat16
    return pl.pallas_call(
        functools.partial(pair_kernel, count),
        in_specs=[ANY] * 20 + [VMEM] * 3 + [SMEM, SMEM],
        out_specs=VMEM,
        out_shape=jax.ShapeDtypeStruct((2, TIDS, QIDS), jnp.float32),
        scratch_shapes=[
            pltpu.VMEM((16,) + cots[0].shape[1:], bf),
            pltpu.VMEM((2, count, HW, HALF), bf),
            pltpu.VMEM((8, HW, HALF), bf),
            pltpu.VMEM((8, SEQ, HALF), bf),
            pltpu.SemaphoreType.DMA((20,)),
        ],
        name="pair_scores",
        compiler_params=pltpu.CompilerParams(vmem_limit_bytes=56 * 2**20),
        cost_estimate=pl.CostEstimate(
            flops=2 * 16 * HW * HALF * SEQ * 4, bytes_accessed=20 * 2**20, transcendentals=0
        ),
    )(*acts, *cots, *own_grads, *other_grads, own_fisher, other_fisher, ids.reshape(1, count), query_ids, layers)


def offset_of(y, x):
    return (2 * y + x // 2) % 8


def local(
    train_inputs,
    train_cotangents,
    train_ids,
    query_projection_inputs,
    query_output_cotangents,
    query_ids,
    fisher_diagonal_weight,
    layer_index,
):
    core, z, y = lax.axis_index("core"), lax.axis_index("z"), lax.axis_index("y")
    x = lax.axis_index("xhi") * 2 + lax.axis_index("xlo")
    up = lambda y, x, z, c: (y, x, z + 1, c)
    down = lambda y, x, z, c: (y, x, z - 1, c)
    swap = lambda y, x, z, c: (y, x, z, 1 - c)

    def turn(k, first):
        def to(y, x, z, c):
            return (y, x - k, z, c) if (c == 0) == first else (y - k, x, z, c)

        return to

    own_x = query_projection_inputs[0]
    m1 = send(own_x, up)
    p1 = send(own_x, down)
    a = (2 * y + x // 2 + 4 * core) % 8
    head = 2 * ((z - a) % 8) + x % 2
    unit = lax.dynamic_slice_in_dim(query_output_cotangents[0], head * HW, HW, 1)
    unit = jnp.pad(unit, ((0, -SEQ % 8), (0, 0)))
    unit = send(unit, lambda y, x, z, c: (y, x, z - offset_of(y, x) - 4 * c, c))
    other_fisher = send(fisher_diagonal_weight, swap)
    own_a = train_grad(train_cotangents, train_inputs, 0, CUTS[0])
    m2 = send(m1, up)
    p2 = send(p1, down)
    parts = [unit, send(unit, turn(1, True)), send(unit, turn(-1, True)), send(unit, turn(2, True))]
    other_a = send(own_a, swap)
    own_b = train_grad(train_cotangents, train_inputs, CUTS[0], CUTS[1])
    la, lb = stack(*parts[:2]), stack(*parts[2:])
    m3 = send(m2, up)
    p3 = send(p2, down)
    lpa, lpb = send(la, turn(1, False)), send(lb, turn(1, False))
    lma, lmb = send(la, turn(-1, False)), send(lb, turn(-1, False))
    other_b = send(own_b, swap)
    far = lax.select(core == 0, m3, p3)
    f4 = send(far, lambda y, x, z, c: (y, x, z + 1 - 2 * c, c))
    l2a = send(lpa, turn(1, False))
    l2b = send(lmb, turn(-1, False))
    buckets = pair_scores(
        (own_x, p1, p2, p3, f4, m3, m2, m1),
        (la, lb, lpa, lpb, lma, lmb, l2a, l2b),
        (own_a, own_b),
        (other_a, other_b),
        fisher_diagonal_weight,
        other_fisher,
        train_ids,
        query_ids,
        layer_index,
    )
    buckets = buckets[0] + send(buckets[1], swap)
    shares = lax.all_to_all(
        buckets.reshape(NY * NXL * NXH, 4, QIDS), ("y", "xlo", "xhi"), 0, 0, tiled=True
    )
    return jnp.sum(shares, axis=0)[:, :, None]


def solution(mesh):
    fine = Mesh(mesh.devices.reshape(NY, NXL, NZ, NC, NXH), AXES)
    dp, tensor, fisher = ("y", "xlo"), ("z", "core"), "xhi"
    in_specs = (
        P(dp, None, fisher),
        P(dp, None, tensor),
        P(dp),
        P(tensor, None, fisher),
        P(tensor, None, None),
        P(),
        P(None, tensor, fisher),
        P(),
    )
    out_specs = P(("y", "xlo", "xhi"), None, tensor)
    return jax.shard_map(local, mesh=fine, in_specs=in_specs, out_specs=out_specs, check_vma=False)
```

```python
import functools
import math

import jax
import jax.numpy as jnp
from jax import lax
from jax.experimental import pallas as pl
from jax.experimental.pallas import tpu as pltpu
from jax.sharding import Mesh, PartitionSpec as P

D = 1280
HEAD_DIM = 80
SEQ = 257
BODY = 256
TIDS = 64
QIDS = 16
HW = 3 * HEAD_DIM
HALF = D // 2
ROWS = 16
CUTS = (11, 11)
NY, NXL, NZ, NC, NXH = 4, 2, 8, 2, 2
AXES = ("y", "xlo", "z", "core", "xhi")
SCALE = 1.0 / (SEQ * math.sqrt(HW * D))
ANY = pl.BlockSpec(memory_space=pl.ANY)
VMEM = pl.BlockSpec(memory_space=pltpu.VMEM)
SMEM = pl.BlockSpec(memory_space=pltpu.SMEM)


def flat(y, x, z, c):
    return (((y % 4) * NXL + (x % 4) % 2) * NZ + z % NZ) * NC * NXH + (c % 2) * NXH + (x % 4) // 2


def send(value, to):
    places = [(y, x, z, c) for y in range(4) for x in range(4) for z in range(NZ) for c in range(2)]
    return lax.ppermute(value, AXES, [(flat(*p), flat(*to(*p))) for p in places])


def outer_sum(cot, act):
    body = lax.dot_general(
        cot[:BODY], act[:BODY], (((0,), (0,)), ((), ())), preferred_element_type=jnp.float32
    )
    column = jnp.transpose(cot[BODY:SEQ].astype(jnp.float32))
    return body + column * act[BODY:SEQ].astype(jnp.float32)


def train_kernel(first, group, cot_hbm, act_hbm, out_ref, cot, act, sems):
    count = out_ref.shape[0]
    copies = []
    for i in range(0, count, group):
        size = min(group, count - i)
        src, dst = pl.ds(first + i, size), pl.ds(i, size)
        pair = (
            pltpu.make_async_copy(cot_hbm.at[src], cot.at[dst], sems.at[0, i // group]),
            pltpu.make_async_copy(act_hbm.at[src], act.at[dst], sems.at[1, i // group]),
        )
        copies.append((i, size, pair))
        for c in pair:
            c.start()
    for i, size, pair in copies:
        for c in pair:
            c.wait()
        for j in range(i, i + size):
            out_ref[j] = outer_sum(cot[j], act[j]).astype(jnp.bfloat16)


def train_grad(cot, act, first, count):
    group = 2
    return pl.pallas_call(
        functools.partial(train_kernel, first, group),
        in_specs=[ANY, ANY],
        out_specs=VMEM,
        out_shape=jax.ShapeDtypeStruct((count, HW, HALF), jnp.bfloat16),
        scratch_shapes=[
            pltpu.VMEM((count, SEQ, HW), jnp.bfloat16),
            pltpu.VMEM((count, SEQ, HALF), jnp.bfloat16),
            pltpu.SemaphoreType.DMA((2, -(-count // group))),
        ],
        name="train_grad",
        compiler_params=pltpu.CompilerParams(vmem_limit_bytes=58 * 2**20),
        cost_estimate=pl.CostEstimate(
            flops=2 * count * HW * HALF * SEQ * 4,
            bytes_accessed=2 * count * (SEQ * (HW + HALF) + HW * HALF),
            transcendentals=0,
        ),
    )(cot, act)


def turned_sum(turned, act):
    body = lax.dot_general(
        turned[:HW], act[:BODY], (((1,), (0,)), ((), ())), preferred_element_type=jnp.float32
    )
    column = jnp.transpose(turned[HW : HW + 1].astype(jnp.float32))[:HW]
    return body + column * act[BODY:SEQ].astype(jnp.float32)


def pack_kernel(cot_ref, out_ref):
    out_ref[:HW] = jnp.transpose(cot_ref[:BODY])
    last = jnp.broadcast_to(cot_ref[BODY:SEQ], (8, HW))
    out_ref[HW:] = jnp.concatenate([last, jnp.zeros((8, BODY - HW), last.dtype)], axis=1)


def pack(cot):
    return pl.pallas_call(
        pack_kernel,
        in_specs=[VMEM],
        out_specs=VMEM,
        out_shape=jax.ShapeDtypeStruct((HW + 8, BODY), cot.dtype),
        name="pack",
        compiler_params=pltpu.CompilerParams(vmem_limit_bytes=4 * 2**20),
    )(cot)


def stack_kernel(*refs):
    *sources, out = refs
    for i, ref in enumerate(sources):
        out[i] = ref[...]


def stack(*parts):
    return pl.pallas_call(
        stack_kernel,
        in_specs=[VMEM] * len(parts),
        out_specs=VMEM,
        out_shape=jax.ShapeDtypeStruct((len(parts),) + parts[0].shape, parts[0].dtype),
        name="stack",
        compiler_params=pltpu.CompilerParams(vmem_limit_bytes=4 * 2**20),
    )(*parts)


def pair_kernel(count_train, *refs):
    acts, refs = refs[:8], refs[8:]
    cots, refs = refs[:8], refs[8:]
    grads, refs = refs[:4], refs[4:]
    own_fisher, other_fisher, ids_ref, query_ids, layer_index, out_ref = refs[:6]
    cot, grad, weighted, act, chosen, sems = refs[6:]
    core, z, y = lax.axis_index("core"), lax.axis_index("z"), lax.axis_index("y")
    x = lax.axis_index("xhi") * 2 + lax.axis_index("xlo")
    first = []
    for k, ref in enumerate(acts):
        first.append(pltpu.make_async_copy(ref, act.at[k], sems.at[k]))
    for i, ref in enumerate(cots):
        first.append(pltpu.make_async_copy(ref, cot.at[pl.ds(2 * i, 2)], sems.at[8 + i]))
    for e, ref in enumerate((own_fisher, other_fisher)):
        layer = layer_index[2 * z + (core if e == 0 else 1 - core)]
        first.append(pltpu.make_async_copy(ref.at[layer], chosen.at[e], sems.at[16 + e]))
    later = []
    for i, ref in enumerate(grads):
        e, rows = i // 2, pl.ds((i % 2) * CUTS[0], ref.shape[0])
        later.append(pltpu.make_async_copy(ref, grad.at[e, rows], sems.at[18 + i]))
    for c in first + later:
        c.start()
    train_hot = (
        lax.broadcasted_iota(jnp.int32, (TIDS, count_train), 0) == ids_ref[...]
    ).astype(jnp.float32)
    column = lax.broadcasted_iota(jnp.int32, (8 * ROWS, QIDS), 0)
    wanted = jnp.zeros((8 * ROWS, QIDS), jnp.int32)
    for k in range(8):
        one = query_ids[2 * lax.rem(z + k, 8) + core]
        wanted = jnp.where(column // ROWS == k, one, wanted)
    query_hot = (lax.broadcasted_iota(jnp.int32, (8 * ROWS, QIDS), 1) == wanted).astype(jnp.float32)
    row = lax.broadcasted_iota(jnp.int32, (count_train * ROWS, 8 * ROWS), 0)
    col = lax.broadcasted_iota(jnp.int32, (count_train * ROWS, 8 * ROWS), 1)
    same = lax.rem(row, ROWS) == lax.rem(col, ROWS)

    def slot(d):
        d = lax.rem(d + 4, 4)
        return jnp.where(d == 2, 3, jnp.where(d == 3, 2, d))

    for c in first:
        c.wait()
    for e in range(2):
        parity = core if e == 0 else 1 - core
        fisher = chosen[e].astype(jnp.float32)
        for k in range(8):
            t = lax.rem(k + 4 * core, 8)
            dy, dx = slot(t // 2 - y), slot(lax.rem(t, 2) * 2 + parity - x)
            unit = jnp.where(core == 0, dy * 4 + dx, dx * 4 + dy)
            weighted[k] = (fisher * turned_sum(cot[unit], act[k])).astype(jnp.bfloat16)
        for c in later[2 * e : 2 * e + 2]:
            c.wait()
        total = jnp.zeros((count_train * ROWS, 8 * ROWS), jnp.float32)
        for r in range(0, HW, ROWS):
            lhs = grad[e, :, r : r + ROWS, :].reshape(count_train * ROWS, HALF)
            rhs = weighted[:, r : r + ROWS, :].reshape(8 * ROWS, HALF)
            total += lax.dot_general(
                lhs, rhs, (((1,), (1,)), ((), ())), preferred_element_type=jnp.float32
            )
        total = jnp.where(same, total, 0.0).reshape(count_train, ROWS, 8 * ROWS).sum(axis=1) * SCALE
        total = jnp.dot(
            total, query_hot, precision=lax.Precision.HIGHEST, preferred_element_type=jnp.float32
        )
        total = jnp.dot(
            train_hot, total, precision=lax.Precision.HIGHEST, preferred_element_type=jnp.float32
        )
        for i in range(TIDS // 4):
            out_ref[2 * i + parity] = total[4 * i : 4 * i + 4]


def pair_scores(acts, cots, grads, own_fisher, other_fisher, ids, query_ids, layers):
    count = ids.shape[0]
    bf = jnp.bfloat16
    return pl.pallas_call(
        functools.partial(pair_kernel, count),
        in_specs=[ANY] * 22 + [VMEM, SMEM, SMEM],
        out_specs=VMEM,
        out_shape=jax.ShapeDtypeStruct((TIDS // 2, 4, QIDS), jnp.float32),
        scratch_shapes=[
            pltpu.VMEM((16,) + cots[0].shape[1:], bf),
            pltpu.VMEM((2, count, HW, HALF), bf),
            pltpu.VMEM((8, HW, HALF), bf),
            pltpu.VMEM((8, SEQ, HALF), bf),
            pltpu.VMEM((2, HW, HALF), bf),
            pltpu.SemaphoreType.DMA((22,)),
        ],
        name="pair_scores",
        compiler_params=pltpu.CompilerParams(vmem_limit_bytes=56 * 2**20),
        cost_estimate=pl.CostEstimate(
            flops=2 * 16 * HW * HALF * SEQ * 4, bytes_accessed=20 * 2**20, transcendentals=0
        ),
    )(*acts, *cots, *grads, own_fisher, other_fisher, ids.reshape(1, count), query_ids, layers)


def offset_of(y, x):
    return (2 * y + x // 2) % 8


def local(
    train_inputs,
    train_cotangents,
    train_ids,
    query_projection_inputs,
    query_output_cotangents,
    query_ids,
    fisher_diagonal_weight,
    layer_index,
):
    core, z, y = lax.axis_index("core"), lax.axis_index("z"), lax.axis_index("y")
    x = lax.axis_index("xhi") * 2 + lax.axis_index("xlo")
    up = lambda y, x, z, c: (y, x, z + 1, c)
    down = lambda y, x, z, c: (y, x, z - 1, c)
    swap = lambda y, x, z, c: (y, x, z, 1 - c)

    def turn(k, first):
        def to(y, x, z, c):
            return (y, x - k, z, c) if (c == 0) == first else (y - k, x, z, c)

        return to

    own_x = query_projection_inputs[0]
    m1 = send(own_x, up)
    p1 = send(own_x, down)
    a = (2 * y + x // 2 + 4 * core) % 8
    head = 2 * ((z - a) % 8) + x % 2
    unit = lax.dynamic_slice_in_dim(query_output_cotangents[0], head * HW, HW, 1)
    unit = pack(unit)
    unit = send(unit, lambda y, x, z, c: (y, x, z - offset_of(y, x) - 4 * c, c))
    other_fisher = send(fisher_diagonal_weight, swap)
    own_a = train_grad(train_cotangents, train_inputs, 0, CUTS[0])
    m2 = send(m1, up)
    p2 = send(p1, down)
    parts = [unit, send(unit, turn(1, True)), send(unit, turn(-1, True)), send(unit, turn(2, True))]
    other_a = send(own_a, swap)
    own_b = train_grad(train_cotangents, train_inputs, CUTS[0], CUTS[1])
    other_b = send(own_b, swap)
    la, lb = stack(*parts[:2]), stack(*parts[2:])
    m3 = send(m2, up)
    p3 = send(p2, down)
    lpa, lpb = send(la, turn(1, False)), send(lb, turn(1, False))
    lma, lmb = send(la, turn(-1, False)), send(lb, turn(-1, False))
    far = lax.select(core == 0, m3, p3)
    f4 = send(far, lambda y, x, z, c: (y, x, z + 1 - 2 * c, c))
    l2a = send(lpa, turn(1, False))
    l2b = send(lmb, turn(-1, False))
    buckets = pair_scores(
        (own_x, p1, p2, p3, f4, m3, m2, m1),
        (la, lb, lpa, lpb, lma, lmb, l2a, l2b),
        (own_a, own_b, other_a, other_b),
        fisher_diagonal_weight,
        other_fisher,
        train_ids,
        query_ids,
        layer_index,
    )
    shares = lax.all_to_all(buckets, ("y", "xlo", "xhi", "core"), 0, 0, tiled=True)
    return jnp.sum(shares, axis=0)[:, :, None]


def solution(mesh):
    fine = Mesh(mesh.devices.reshape(NY, NXL, NZ, NC, NXH), AXES)
    dp, tensor, fisher = ("y", "xlo"), ("z", "core"), "xhi"
    in_specs = (
        P(dp, None, fisher),
        P(dp, None, tensor),
        P(dp),
        P(tensor, None, fisher),
        P(tensor, None, None),
        P(),
        P(None, tensor, fisher),
        P(),
    )
    out_specs = P(("y", "xlo", "xhi"), None, tensor)
    return jax.shard_map(local, mesh=fine, in_specs=in_specs, out_specs=out_specs, check_vma=False)
```

```python
import functools
import math

import jax
import jax.numpy as jnp
from jax import lax
from jax.experimental import pallas as pl
from jax.experimental.pallas import tpu as pltpu
from jax.sharding import Mesh, PartitionSpec as P

D = 1280
HEAD_DIM = 80
HEADS = 16
SEQ = 257
BODY = 256
TIDS = 64
QIDS = 16
HW = 3 * HEAD_DIM
HALF = D // 2
ROWS = 16
CUTS = (10, 12)
NY, NXL, NZ, NC, NXH = 4, 2, 8, 2, 2
AXES = ("y", "xlo", "z", "core", "xhi")
SCALE = 1.0 / (SEQ * math.sqrt(HW * D))
ANY = pl.BlockSpec(memory_space=pl.ANY)
VMEM = pl.BlockSpec(memory_space=pltpu.VMEM)


def flat(y, x, z, c):
    return (((y % 4) * NXL + (x % 4) % 2) * NZ + z % NZ) * NC * NXH + (c % 2) * NXH + (x % 4) // 2


def send(value, to):
    places = [(y, x, z, c) for y in range(4) for x in range(4) for z in range(NZ) for c in range(2)]
    return lax.ppermute(value, AXES, [(flat(*p), flat(*to(*p))) for p in places])


def outer_sum(cot, act):
    body = lax.dot_general(
        cot[:BODY], act[:BODY], (((0,), (0,)), ((), ())), preferred_element_type=jnp.float32
    )
    column = jnp.transpose(cot[BODY:SEQ].astype(jnp.float32))
    return body + column * act[BODY:SEQ].astype(jnp.float32)


def train_kernel(first, group, cot_hbm, act_hbm, out_hbm, cot, act, out, sems):
    count = out.shape[0]
    copies = []
    for i in range(0, count, group):
        src, dst = pl.ds(first + i, group), pl.ds(i, group)
        copies.append(
            (
                pltpu.make_async_copy(cot_hbm.at[src], cot.at[dst], sems.at[0, i // group]),
                pltpu.make_async_copy(act_hbm.at[src], act.at[dst], sems.at[1, i // group]),
                pltpu.make_async_copy(out.at[dst], out_hbm.at[dst], sems.at[2, i // group]),
            )
        )
    for c in copies:
        c[0].start()
        c[1].start()
    for i, c in enumerate(copies):
        c[0].wait()
        c[1].wait()
        for j in range(i * group, (i + 1) * group):
            out[j] = outer_sum(cot[j], act[j]).astype(jnp.bfloat16)
        c[2].start()
    for c in copies:
        c[2].wait()


def train_grad(cot, act, first, count):
    group = 2
    return pl.pallas_call(
        functools.partial(train_kernel, first, group),
        in_specs=[ANY, ANY],
        out_specs=ANY,
        out_shape=jax.ShapeDtypeStruct((count, HW, HALF), jnp.bfloat16),
        scratch_shapes=[
            pltpu.VMEM((count, SEQ, HW), jnp.bfloat16),
            pltpu.VMEM((count, SEQ, HALF), jnp.bfloat16),
            pltpu.VMEM((count, HW, HALF), jnp.bfloat16),
            pltpu.SemaphoreType.DMA((3, count // group)),
        ],
        name="train_grad",
        compiler_params=pltpu.CompilerParams(vmem_limit_bytes=58 * 2**20),
        cost_estimate=pl.CostEstimate(
            flops=2 * count * HW * HALF * SEQ * 4,
            bytes_accessed=2 * count * (SEQ * (HW + HALF) + HW * HALF),
            transcendentals=0,
        ),
    )(cot, act)


def turned_sum(turned, act):
    body = lax.dot_general(
        turned[:HW], act[:BODY], (((1,), (0,)), ((), ())), preferred_element_type=jnp.float32
    )
    column = jnp.transpose(turned[HW : HW + 1].astype(jnp.float32))[:HW]
    return body + column * act[BODY:SEQ].astype(jnp.float32)


def pack_kernel(cot_ref, out_ref):
    out_ref[:HW] = jnp.transpose(cot_ref[:BODY])
    last = jnp.broadcast_to(cot_ref[BODY:SEQ], (8, HW))
    out_ref[HW:] = jnp.concatenate([last, jnp.zeros((8, BODY - HW), last.dtype)], axis=1)


def pack(cot):
    return pl.pallas_call(
        pack_kernel,
        in_specs=[VMEM],
        out_specs=VMEM,
        out_shape=jax.ShapeDtypeStruct((HW + 8, BODY), cot.dtype),
        name="pack",
        compiler_params=pltpu.CompilerParams(vmem_limit_bytes=4 * 2**20),
    )(cot)


def stack_kernel(*refs):
    *sources, out = refs
    for i, ref in enumerate(sources):
        out[i] = ref[...]


def stack(*parts):
    return pl.pallas_call(
        stack_kernel,
        in_specs=[VMEM] * len(parts),
        out_specs=VMEM,
        out_shape=jax.ShapeDtypeStruct((len(parts),) + parts[0].shape, parts[0].dtype),
        name="stack",
        compiler_params=pltpu.CompilerParams(vmem_limit_bytes=4 * 2**20),
    )(*parts)


def pair_kernel(count_train, *refs):
    acts, refs = refs[:8], refs[8:]
    cots, refs = refs[:4], refs[4:]
    grads, refs = refs[:4], refs[4:]
    own_fisher, other_fisher, table_ref, out_ref = refs[:4]
    cot, grad, weighted, act, fishers, table, sems = refs[4:]
    core, z, y = lax.axis_index("core"), lax.axis_index("z"), lax.axis_index("y")
    x = lax.axis_index("xhi") * 2 + lax.axis_index("xlo")
    first = []
    for k, ref in enumerate(acts):
        first.append(pltpu.make_async_copy(ref, act.at[k], sems.at[k]))
    for i, ref in enumerate(cots):
        first.append(pltpu.make_async_copy(ref, cot.at[pl.ds(4 * i, 4)], sems.at[8 + i]))
    for e, ref in enumerate((own_fisher, other_fisher)):
        first.append(pltpu.make_async_copy(ref, fishers.at[e], sems.at[16 + e]))
    later = []
    for i, ref in enumerate(grads):
        e, rows = i // 2, pl.ds((i % 2) * CUTS[0], ref.shape[0])
        later.append(pltpu.make_async_copy(ref, grad.at[e, rows], sems.at[18 + i]))
    numbers = pltpu.make_async_copy(table_ref, table, sems.at[22])
    for c in [numbers] + first + later:
        c.start()
    numbers.wait()
    place = lax.broadcasted_iota(jnp.int32, (TIDS, count_train), 1)
    ids = jnp.zeros((TIDS, count_train), jnp.int32)
    for n in range(count_train):
        ids = jnp.where(place == n, table[2 * HEADS + n], ids)
    train_hot = (lax.broadcasted_iota(jnp.int32, (TIDS, count_train), 0) == ids).astype(jnp.float32)
    column = lax.broadcasted_iota(jnp.int32, (8 * ROWS, QIDS), 0)
    wanted = jnp.zeros((8 * ROWS, QIDS), jnp.int32)
    for k in range(8):
        one = table[HEADS + 2 * lax.rem(z + k, 8) + core]
        wanted = jnp.where(column // ROWS == k, one, wanted)
    query_hot = (lax.broadcasted_iota(jnp.int32, (8 * ROWS, QIDS), 1) == wanted).astype(jnp.float32)
    row = lax.broadcasted_iota(jnp.int32, (count_train * ROWS, 8 * ROWS), 0)
    col = lax.broadcasted_iota(jnp.int32, (count_train * ROWS, 8 * ROWS), 1)
    same = lax.rem(row, ROWS) == lax.rem(col, ROWS)

    def slot(d):
        d = lax.rem(d + 4, 4)
        return jnp.where(d == 2, 3, jnp.where(d == 3, 2, d))

    for c in first:
        c.wait()
    for e in range(2):
        parity = core if e == 0 else 1 - core
        fisher = fishers[e, table[2 * z + parity]].astype(jnp.float32)
        for k in range(8):
            t = lax.rem(k + 4 * core, 8)
            dy, dx = slot(t // 2 - y), slot(lax.rem(t, 2) * 2 + parity - x)
            unit = jnp.where(core == 0, dy * 4 + dx, dx * 4 + dy)
            weighted[k] = (fisher * turned_sum(cot[unit], act[k])).astype(jnp.bfloat16)
        for c in later[2 * e : 2 * e + 2]:
            c.wait()
        total = jnp.zeros((count_train * ROWS, 8 * ROWS), jnp.float32)
        for r in range(0, HW, ROWS):
            lhs = grad[e, :, r : r + ROWS, :].reshape(count_train * ROWS, HALF)
            rhs = weighted[:, r : r + ROWS, :].reshape(8 * ROWS, HALF)
            total += lax.dot_general(
                lhs, rhs, (((1,), (1,)), ((), ())), preferred_element_type=jnp.float32
            )
        total = jnp.where(same, total, 0.0).reshape(count_train, ROWS, 8 * ROWS).sum(axis=1) * SCALE
        total = jnp.dot(
            total, query_hot, precision=lax.Precision.HIGHEST, preferred_element_type=jnp.float32
        )
        total = jnp.dot(
            train_hot, total, precision=lax.Precision.HIGHEST, preferred_element_type=jnp.float32
        )
        for i in range(TIDS // 4):
            out_ref[2 * i + parity] = total[4 * i : 4 * i + 4]


def pair_scores(acts, cots, grads, own_fisher, other_fisher, ids, query_ids, layers):
    count = ids.shape[0]
    bf = jnp.bfloat16
    table = jnp.concatenate([layers, query_ids, ids])
    table = jnp.pad(table, (0, 128 - table.shape[0]))
    return pl.pallas_call(
        functools.partial(pair_kernel, count),
        in_specs=[ANY] * 19,
        out_specs=VMEM,
        out_shape=jax.ShapeDtypeStruct((TIDS // 2, 4, QIDS), jnp.float32),
        scratch_shapes=[
            pltpu.VMEM((16,) + cots[0].shape[1:], bf),
            pltpu.VMEM((2, count, HW, HALF), bf),
            pltpu.VMEM((8, HW, HALF), bf),
            pltpu.VMEM((8, SEQ, HALF), bf),
            pltpu.VMEM((2,) + own_fisher.shape, bf),
            pltpu.SMEM((128,), jnp.int32),
            pltpu.SemaphoreType.DMA((23,)),
        ],
        name="pair_scores",
        compiler_params=pltpu.CompilerParams(vmem_limit_bytes=56 * 2**20),
        cost_estimate=pl.CostEstimate(
            flops=2 * 16 * HW * HALF * SEQ * 4, bytes_accessed=20 * 2**20, transcendentals=0
        ),
    )(*acts, *cots, *grads, own_fisher, other_fisher, table)


def offset_of(y, x):
    return (2 * y + x // 2) % 8


def local(
    train_inputs,
    train_cotangents,
    train_ids,
    query_projection_inputs,
    query_output_cotangents,
    query_ids,
    fisher_diagonal_weight,
    layer_index,
):
    core, z, y = lax.axis_index("core"), lax.axis_index("z"), lax.axis_index("y")
    x = lax.axis_index("xhi") * 2 + lax.axis_index("xlo")
    up = lambda y, x, z, c: (y, x, z + 1, c)
    down = lambda y, x, z, c: (y, x, z - 1, c)
    swap = lambda y, x, z, c: (y, x, z, 1 - c)

    def turn(k, first):
        def to(y, x, z, c):
            return (y, x - k, z, c) if (c == 0) == first else (y - k, x, z, c)

        return to

    own_x = query_projection_inputs[0]
    m1 = send(own_x, up)
    p1 = send(own_x, down)
    a = (2 * y + x // 2 + 4 * core) % 8
    head = 2 * ((z - a) % 8) + x % 2
    unit = lax.dynamic_slice_in_dim(query_output_cotangents[0], head * HW, HW, 1)
    unit = pack(unit)
    unit = send(unit, lambda y, x, z, c: (y, x, z - offset_of(y, x) - 4 * c, c))
    other_fisher = send(fisher_diagonal_weight, swap)
    own_a = train_grad(train_cotangents, train_inputs, 0, CUTS[0])
    m2 = send(m1, up)
    p2 = send(p1, down)
    parts = [unit, send(unit, turn(1, True)), send(unit, turn(-1, True)), send(unit, turn(2, True))]
    other_a = send(own_a, swap)
    line = stack(*parts)
    m3 = send(m2, up)
    p3 = send(p2, down)
    lp = send(line, turn(1, False))
    lm = send(line, turn(-1, False))
    own_b = train_grad(train_cotangents, train_inputs, CUTS[0], CUTS[1])
    other_b = send(own_b, swap)
    l2 = send(lp, turn(1, False))
    far = lax.select(core == 0, m3, p3)
    f4 = send(far, lambda y, x, z, c: (y, x, z + 1 - 2 * c, c))
    buckets = pair_scores(
        (own_x, p1, p2, p3, f4, m3, m2, m1),
        (line, lp, lm, l2),
        (own_a, own_b, other_a, other_b),
        fisher_diagonal_weight,
        other_fisher,
        train_ids,
        query_ids,
        layer_index,
    )
    shares = lax.all_to_all(buckets, ("y", "xlo", "xhi", "core"), 0, 0, tiled=True)
    return jnp.sum(shares, axis=0)[:, :, None]


def solution(mesh):
    fine = Mesh(mesh.devices.reshape(NY, NXL, NZ, NC, NXH), AXES)
    dp, tensor, fisher = ("y", "xlo"), ("z", "core"), "xhi"
    in_specs = (
        P(dp, None, fisher),
        P(dp, None, tensor),
        P(dp),
        P(tensor, None, fisher),
        P(tensor, None, None),
        P(),
        P(None, tensor, fisher),
        P(),
    )
    out_specs = P(("y", "xlo", "xhi"), None, tensor)
    return jax.shard_map(local, mesh=fine, in_specs=in_specs, out_specs=out_specs, check_vma=False)
```

```python
import functools
import math

import jax
import jax.numpy as jnp
from jax import lax
from jax.experimental import pallas as pl
from jax.experimental.pallas import tpu as pltpu
from jax.sharding import Mesh, PartitionSpec as P

D = 1280
HEAD_DIM = 80
HEADS = 16
SEQ = 257
BODY = 256
TIDS = 64
QIDS = 16
HW = 3 * HEAD_DIM
HALF = D // 2
ROWS = 16
CUTS = (8, 6, 8)
NY, NXL, NZ, NC, NXH = 4, 2, 8, 2, 2
AXES = ("y", "xlo", "z", "core", "xhi")
SCALE = 1.0 / (SEQ * math.sqrt(HW * D))
ANY = pl.BlockSpec(memory_space=pl.ANY)
VMEM = pl.BlockSpec(memory_space=pltpu.VMEM)


def flat(y, x, z, c):
    return (((y % 4) * NXL + (x % 4) % 2) * NZ + z % NZ) * NC * NXH + (c % 2) * NXH + (x % 4) // 2


def send(value, to):
    places = [(y, x, z, c) for y in range(4) for x in range(4) for z in range(NZ) for c in range(2)]
    return lax.ppermute(value, AXES, [(flat(*p), flat(*to(*p))) for p in places])


def outer_sum(cot, act):
    body = lax.dot_general(
        cot[:BODY], act[:BODY], (((0,), (0,)), ((), ())), preferred_element_type=jnp.float32
    )
    column = jnp.transpose(cot[BODY:SEQ].astype(jnp.float32))
    return body + column * act[BODY:SEQ].astype(jnp.float32)


def train_kernel(first, group, cot_hbm, act_hbm, out_hbm, cot, act, out, sems):
    count = out.shape[0]
    copies = []
    for i in range(0, count, group):
        src, dst = pl.ds(first + i, group), pl.ds(i, group)
        copies.append(
            (
                pltpu.make_async_copy(cot_hbm.at[src], cot.at[dst], sems.at[0, i // group]),
                pltpu.make_async_copy(act_hbm.at[src], act.at[dst], sems.at[1, i // group]),
                pltpu.make_async_copy(out.at[dst], out_hbm.at[dst], sems.at[2, i // group]),
            )
        )
    for c in copies:
        c[0].start()
        c[1].start()
    for i, c in enumerate(copies):
        c[0].wait()
        c[1].wait()
        for j in range(i * group, (i + 1) * group):
            out[j] = outer_sum(cot[j], act[j]).astype(jnp.bfloat16)
        c[2].start()
    for c in copies:
        c[2].wait()


def train_grad(cot, act, first, count):
    group = 2
    return pl.pallas_call(
        functools.partial(train_kernel, first, group),
        in_specs=[ANY, ANY],
        out_specs=ANY,
        out_shape=jax.ShapeDtypeStruct((count, HW, HALF), jnp.bfloat16),
        scratch_shapes=[
            pltpu.VMEM((count, SEQ, HW), jnp.bfloat16),
            pltpu.VMEM((count, SEQ, HALF), jnp.bfloat16),
            pltpu.VMEM((count, HW, HALF), jnp.bfloat16),
            pltpu.SemaphoreType.DMA((3, count // group)),
        ],
        name="train_grad",
        compiler_params=pltpu.CompilerParams(vmem_limit_bytes=58 * 2**20),
        cost_estimate=pl.CostEstimate(
            flops=2 * count * HW * HALF * SEQ * 4,
            bytes_accessed=2 * count * (SEQ * (HW + HALF) + HW * HALF),
            transcendentals=0,
        ),
    )(cot, act)


def turned_sum(turned, act):
    body = lax.dot_general(
        turned[:HW], act[:BODY], (((1,), (0,)), ((), ())), preferred_element_type=jnp.float32
    )
    column = jnp.transpose(turned[HW : HW + 1].astype(jnp.float32))[:HW]
    return body + column * act[BODY:SEQ].astype(jnp.float32)


def pack_kernel(cot_ref, out_ref):
    out_ref[:HW] = jnp.transpose(cot_ref[:BODY])
    last = jnp.broadcast_to(cot_ref[BODY:SEQ], (8, HW))
    out_ref[HW:] = jnp.concatenate([last, jnp.zeros((8, BODY - HW), last.dtype)], axis=1)


def pack(cot):
    return pl.pallas_call(
        pack_kernel,
        in_specs=[VMEM],
        out_specs=VMEM,
        out_shape=jax.ShapeDtypeStruct((HW + 8, BODY), cot.dtype),
        name="pack",
        compiler_params=pltpu.CompilerParams(vmem_limit_bytes=4 * 2**20),
    )(cot)


def stack_kernel(*refs):
    *sources, out = refs
    for i, ref in enumerate(sources):
        out[i] = ref[...]


def stack(*parts):
    return pl.pallas_call(
        stack_kernel,
        in_specs=[VMEM] * len(parts),
        out_specs=VMEM,
        out_shape=jax.ShapeDtypeStruct((len(parts),) + parts[0].shape, parts[0].dtype),
        name="stack",
        compiler_params=pltpu.CompilerParams(vmem_limit_bytes=4 * 2**20),
    )(*parts)


def pair_kernel(count_train, *refs):
    acts, refs = refs[:8], refs[8:]
    cots, refs = refs[:4], refs[4:]
    grads, refs = refs[:6], refs[6:]
    own_fisher, other_fisher, table_ref, out_ref = refs[:4]
    cot, grad, weighted, act, fishers, table, sems = refs[4:]
    core, z, y = lax.axis_index("core"), lax.axis_index("z"), lax.axis_index("y")
    x = lax.axis_index("xhi") * 2 + lax.axis_index("xlo")
    first = []
    for k, ref in enumerate(acts):
        first.append(pltpu.make_async_copy(ref, act.at[k], sems.at[k]))
    for i, ref in enumerate(cots):
        first.append(pltpu.make_async_copy(ref, cot.at[pl.ds(4 * i, 4)], sems.at[8 + i]))
    for e, ref in enumerate((own_fisher, other_fisher)):
        first.append(pltpu.make_async_copy(ref, fishers.at[e], sems.at[16 + e]))
    later = []
    for i, ref in enumerate(grads):
        e, rows = i // 3, pl.ds(sum(CUTS[: i % 3]), ref.shape[0])
        later.append(pltpu.make_async_copy(ref, grad.at[e, rows], sems.at[18 + i]))
    numbers = pltpu.make_async_copy(table_ref, table, sems.at[24])
    for c in [numbers] + first + later:
        c.start()
    numbers.wait()
    place = lax.broadcasted_iota(jnp.int32, (TIDS, count_train), 1)
    ids = jnp.zeros((TIDS, count_train), jnp.int32)
    for n in range(count_train):
        ids = jnp.where(place == n, table[2 * HEADS + n], ids)
    train_hot = (lax.broadcasted_iota(jnp.int32, (TIDS, count_train), 0) == ids).astype(jnp.float32)
    column = lax.broadcasted_iota(jnp.int32, (8 * ROWS, QIDS), 0)
    wanted = jnp.zeros((8 * ROWS, QIDS), jnp.int32)
    for k in range(8):
        one = table[HEADS + 2 * lax.rem(z + k, 8) + core]
        wanted = jnp.where(column // ROWS == k, one, wanted)
    query_hot = (lax.broadcasted_iota(jnp.int32, (8 * ROWS, QIDS), 1) == wanted).astype(jnp.float32)
    row = lax.broadcasted_iota(jnp.int32, (count_train * ROWS, 8 * ROWS), 0)
    col = lax.broadcasted_iota(jnp.int32, (count_train * ROWS, 8 * ROWS), 1)
    same = lax.rem(row, ROWS) == lax.rem(col, ROWS)

    def slot(d):
        d = lax.rem(d + 4, 4)
        return jnp.where(d == 2, 3, jnp.where(d == 3, 2, d))

    for c in first:
        c.wait()
    for e in range(2):
        parity = core if e == 0 else 1 - core
        fisher = fishers[e, table[2 * z + parity]].astype(jnp.float32)
        for k in range(8):
            t = lax.rem(k + 4 * core, 8)
            dy, dx = slot(t // 2 - y), slot(lax.rem(t, 2) * 2 + parity - x)
            unit = jnp.where(core == 0, dy * 4 + dx, dx * 4 + dy)
            weighted[k] = (fisher * turned_sum(cot[unit], act[k])).astype(jnp.bfloat16)
        for c in later[3 * e : 3 * e + 3]:
            c.wait()
        total = jnp.zeros((count_train * ROWS, 8 * ROWS), jnp.float32)
        for r in range(0, HW, ROWS):
            lhs = grad[e, :, r : r + ROWS, :].reshape(count_train * ROWS, HALF)
            rhs = weighted[:, r : r + ROWS, :].reshape(8 * ROWS, HALF)
            total += lax.dot_general(
                lhs, rhs, (((1,), (1,)), ((), ())), preferred_element_type=jnp.float32
            )
        total = jnp.where(same, total, 0.0).reshape(count_train, ROWS, 8 * ROWS).sum(axis=1) * SCALE
        total = jnp.dot(
            total, query_hot, precision=lax.Precision.HIGHEST, preferred_element_type=jnp.float32
        )
        total = jnp.dot(
            train_hot, total, precision=lax.Precision.HIGHEST, preferred_element_type=jnp.float32
        )
        for i in range(TIDS // 4):
            out_ref[2 * i + parity] = total[4 * i : 4 * i + 4]


def pair_scores(acts, cots, grads, own_fisher, other_fisher, ids, query_ids, layers):
    count = ids.shape[0]
    bf = jnp.bfloat16
    table = jnp.concatenate([layers, query_ids, ids])
    table = jnp.pad(table, (0, 128 - table.shape[0]))
    return pl.pallas_call(
        functools.partial(pair_kernel, count),
        in_specs=[ANY] * 21,
        out_specs=VMEM,
        out_shape=jax.ShapeDtypeStruct((TIDS // 2, 4, QIDS), jnp.float32),
        scratch_shapes=[
            pltpu.VMEM((16,) + cots[0].shape[1:], bf),
            pltpu.VMEM((2, count, HW, HALF), bf),
            pltpu.VMEM((8, HW, HALF), bf),
            pltpu.VMEM((8, SEQ, HALF), bf),
            pltpu.VMEM((2,) + own_fisher.shape, bf),
            pltpu.SMEM((128,), jnp.int32),
            pltpu.SemaphoreType.DMA((25,)),
        ],
        name="pair_scores",
        compiler_params=pltpu.CompilerParams(vmem_limit_bytes=56 * 2**20),
        cost_estimate=pl.CostEstimate(
            flops=2 * 16 * HW * HALF * SEQ * 4, bytes_accessed=20 * 2**20, transcendentals=0
        ),
    )(*acts, *cots, *grads, own_fisher, other_fisher, table)


def offset_of(y, x):
    return (2 * y + x // 2) % 8


def local(
    train_inputs,
    train_cotangents,
    train_ids,
    query_projection_inputs,
    query_output_cotangents,
    query_ids,
    fisher_diagonal_weight,
    layer_index,
):
    core, z, y = lax.axis_index("core"), lax.axis_index("z"), lax.axis_index("y")
    x = lax.axis_index("xhi") * 2 + lax.axis_index("xlo")
    up = lambda y, x, z, c: (y, x, z + 1, c)
    down = lambda y, x, z, c: (y, x, z - 1, c)
    swap = lambda y, x, z, c: (y, x, z, 1 - c)

    def turn(k, first):
        def to(y, x, z, c):
            return (y, x - k, z, c) if (c == 0) == first else (y - k, x, z, c)

        return to

    own_x = query_projection_inputs[0]
    m1 = send(own_x, up)
    p1 = send(own_x, down)
    a = (2 * y + x // 2 + 4 * core) % 8
    head = 2 * ((z - a) % 8) + x % 2
    unit = lax.dynamic_slice_in_dim(query_output_cotangents[0], head * HW, HW, 1)
    unit = pack(unit)
    unit = send(unit, lambda y, x, z, c: (y, x, z - offset_of(y, x) - 4 * c, c))
    other_fisher = send(fisher_diagonal_weight, swap)
    own_a = train_grad(train_cotangents, train_inputs, 0, CUTS[0])
    m2 = send(m1, up)
    p2 = send(p1, down)
    parts = [unit, send(unit, turn(1, True)), send(unit, turn(-1, True)), send(unit, turn(2, True))]
    other_a = send(own_a, swap)
    line = stack(*parts)
    m3 = send(m2, up)
    p3 = send(p2, down)
    lp = send(line, turn(1, False))
    lm = send(line, turn(-1, False))
    own_b = train_grad(train_cotangents, train_inputs, CUTS[0], CUTS[1])
    other_b = send(own_b, swap)
    l2 = send(lp, turn(1, False))
    own_c = train_grad(train_cotangents, train_inputs, CUTS[0] + CUTS[1], CUTS[2])
    other_c = send(own_c, swap)
    far = lax.select(core == 0, m3, p3)
    f4 = send(far, lambda y, x, z, c: (y, x, z + 1 - 2 * c, c))
    buckets = pair_scores(
        (own_x, p1, p2, p3, f4, m3, m2, m1),
        (line, lp, lm, l2),
        (own_a, own_b, own_c, other_a, other_b, other_c),
        fisher_diagonal_weight,
        other_fisher,
        train_ids,
        query_ids,
        layer_index,
    )
    shares = lax.all_to_all(buckets, ("y", "xlo", "xhi", "core"), 0, 0, tiled=True)
    return jnp.sum(shares, axis=0)[:, :, None]


def solution(mesh):
    fine = Mesh(mesh.devices.reshape(NY, NXL, NZ, NC, NXH), AXES)
    dp, tensor, fisher = ("y", "xlo"), ("z", "core"), "xhi"
    in_specs = (
        P(dp, None, fisher),
        P(dp, None, tensor),
        P(dp),
        P(tensor, None, fisher),
        P(tensor, None, None),
        P(),
        P(None, tensor, fisher),
        P(),
    )
    out_specs = P(("y", "xlo", "xhi"), None, tensor)
    return jax.shard_map(local, mesh=fine, in_specs=in_specs, out_specs=out_specs, check_vma=False)
```
